32 devices in a mesh: rep: 1 (over z), dp: 32 (over y, x, core).
Axes of the slice: x: 4, y: 4, z: 1, core: 2. Of those that a mesh axis runs over, the one named last changes fastest.
The devices are a block of a 4x4x8 slice.
Arguments:
- tokens: int32 [2, 96], P(None, ('rep', 'dp'))
- start_pos: int32 [96], P(('rep', 'dp'))
- k_cache: bfloat16 [2, 96, 12, 1024, 64], P(None, ('rep', 'dp'))
- v_cache: bfloat16 [2, 96, 12, 1024, 64], P(None, ('rep', 'dp'))
- tok_table: bfloat16 [50272, 768], P('dp')
- pos_table: bfloat16 [2048, 768], P('dp')
- ln1_gain: bfloat16 [2, 768], P(None, 'dp')
- ln1_bias: bfloat16 [2, 768], P(None, 'dp')
- w_q: bfloat16 [2, 768, 768], P(None, 'dp')
- w_k: bfloat16 [2, 768, 768], P(None, 'dp')
- w_v: bfloat16 [2, 768, 768], P(None, 'dp')
- b_q: bfloat16 [2, 768], P(None, 'dp')
- b_k: bfloat16 [2, 768], P(None, 'dp')
- b_v: bfloat16 [2, 768], P(None, 'dp')
- w_o: bfloat16 [2, 768, 768], P(None, 'dp')
- b_o: bfloat16 [2, 768], P(None, 'dp')
- ln2_gain: bfloat16 [2, 768], P(None, 'dp')
- ln2_bias: bfloat16 [2, 768], P(None, 'dp')
- w_fc1: bfloat16 [2, 768, 3072], P(None, 'dp')
- b_fc1: bfloat16 [2, 3072], P(None, 'dp')
- w_fc2: bfloat16 [2, 3072, 768], P(None, 'dp')
- b_fc2: bfloat16 [2, 768], P(None, 'dp')
- lnf_gain: bfloat16 [768], P('dp')
- lnf_bias: bfloat16 [768], P('dp')
Outputs:
- output 1: float32 [2, 96, 50272], P(None, ('rep', 'dp'))
- output 2: bfloat16 [2, 96, 12, 1024, 64], P(None, ('rep', 'dp'))
- output 3: bfloat16 [2, 96, 12, 1024, 64], P(None, ('rep', 'dp'))
All inputs are finite; a program needn't handle non-finite values.
Results may differ from the reference program's by a relative error of at most 0.00434985.
Values are sent between devices in bfloat16 or wider.
A program may use at most 768 MiB of HBM per device.

```python
import jax
import jax.numpy as jnp
from jax import lax

D = 768
HEADS = 12
FF = 3072
VOCAB = 50272
POS = 2048
GROUP = 32
BATCH = 96
CACHE_LEN = 1024
STEPS = 2
LAYERS = 2
HEAD_DIM = D // HEADS
EPS = 1e-5


def setup_inputs(seed: int = 0, part: int = 0) -> dict:
    part_keys = jax.random.split(jax.random.fold_in(jax.random.key(seed), part), 5)
    share_keys = jax.random.split(jax.random.key(seed + 1), 20)

    def normal(key, shape, scale):
        return (jax.random.normal(key, shape, jnp.float32) * scale).astype(jnp.bfloat16)

    def gain(key, shape):
        return (1.0 + 0.3 * jax.random.normal(key, shape, jnp.float32)).astype(jnp.bfloat16)

    shard_rows = VOCAB // GROUP
    count = STEPS * BATCH
    shift = jax.random.randint(part_keys[0], (), 0, GROUP, dtype=jnp.int32)
    shard_ids = (jnp.arange(count, dtype=jnp.int32) + shift) % GROUP
    offsets = jax.random.randint(part_keys[1], (count,), 0, shard_rows, dtype=jnp.int32)
    flat_tok = (shard_ids * shard_rows + offsets).at[0].set(0).at[1].set(VOCAB - 1)
    tokens = flat_tok.reshape(STEPS, BATCH).astype(jnp.int32)
    start_pos = jax.random.randint(part_keys[2], (BATCH,), 0, CACHE_LEN - STEPS + 1, dtype=jnp.int32)
    start_pos = start_pos.at[0].set(0).at[1].set(CACHE_LEN - STEPS)
    cache_shape = (LAYERS, BATCH, HEADS, CACHE_LEN, HEAD_DIM)
    square_shape = (LAYERS, D, D)
    return {
        'tokens': tokens,
        'start_pos': start_pos,
        'k_cache': normal(part_keys[3], cache_shape, 1.0),
        'v_cache': normal(part_keys[4], cache_shape, 1.0),
        'tok_table': normal(share_keys[0], (VOCAB, D), D ** -0.5),
        'pos_table': normal(share_keys[1], (POS, D), D ** -0.5),
        'ln1_gain': gain(share_keys[2], (LAYERS, D)),
        'ln1_bias': normal(share_keys[3], (LAYERS, D), 0.3),
        'w_q': normal(share_keys[4], square_shape, D ** -0.5),
        'w_k': normal(share_keys[5], square_shape, D ** -0.5),
        'w_v': normal(share_keys[6], square_shape, D ** -0.5),
        'b_q': normal(share_keys[7], (LAYERS, D), 0.5),
        'b_k': normal(share_keys[8], (LAYERS, D), 0.5),
        'b_v': normal(share_keys[9], (LAYERS, D), 0.5),
        'w_o': normal(share_keys[10], square_shape, D ** -0.5),
        'b_o': normal(share_keys[11], (LAYERS, D), 0.3),
        'ln2_gain': gain(share_keys[12], (LAYERS, D)),
        'ln2_bias': normal(share_keys[13], (LAYERS, D), 0.3),
        'w_fc1': normal(share_keys[14], (LAYERS, D, FF), D ** -0.5),
        'b_fc1': normal(share_keys[15], (LAYERS, FF), 0.3),
        'w_fc2': normal(share_keys[16], (LAYERS, FF, D), FF ** -0.5),
        'b_fc2': normal(share_keys[17], (LAYERS, D), 0.3),
        'lnf_gain': gain(share_keys[18], (D,)),
        'lnf_bias': normal(share_keys[19], (D,), 0.3),
    }


def layer_norm(resid_in, gain, shift):
    mean = jnp.mean(resid_in, axis=-1, keepdims=True)
    variance = jnp.mean(jnp.square(resid_in - mean), axis=-1, keepdims=True)
    normed = (resid_in - mean) * lax.rsqrt(variance + EPS)
    return (normed * gain.astype(jnp.float32) + shift.astype(jnp.float32)).astype(jnp.bfloat16)


def matmul(left, right):
    return jnp.dot(left, right, preferred_element_type=jnp.float32)


def reference(tokens, start_pos, k_cache, v_cache, tok_table, pos_table, ln1_gain, ln1_bias, w_q, w_k, w_v, b_q, b_k, b_v, w_o, b_o, ln2_gain, ln2_bias, w_fc1, b_fc1, w_fc2, b_fc2, lnf_gain, lnf_bias):
    scale = HEAD_DIM ** -0.5
    slots = jnp.arange(CACHE_LEN, dtype=jnp.int32)

    def one_step(carry, step_in):
        k_layers, v_layers = carry
        step_tok, step_idx = step_in
        cur_pos = start_pos + step_idx
        residual = tok_table[step_tok].astype(jnp.float32) + pos_table[cur_pos].astype(jnp.float32)
        hit_mask = (slots[None, :] == cur_pos[:, None])[:, None, :, None]
        valid = (slots[None, :] <= cur_pos[:, None])[:, None, :]
        new_k = []
        new_v = []
        for layer in range(LAYERS):
            hidden = layer_norm(residual, ln1_gain[layer], ln1_bias[layer])
            query = ((matmul(hidden, w_q[layer]) + b_q[layer].astype(jnp.float32)) * scale).astype(jnp.bfloat16)
            k_fresh = (matmul(hidden, w_k[layer]) + b_k[layer].astype(jnp.float32)).astype(jnp.bfloat16)
            v_fresh = (matmul(hidden, w_v[layer]) + b_v[layer].astype(jnp.float32)).astype(jnp.bfloat16)
            k_layer = jnp.where(hit_mask, k_fresh.reshape(BATCH, HEADS, 1, HEAD_DIM), k_layers[layer])
            v_layer = jnp.where(hit_mask, v_fresh.reshape(BATCH, HEADS, 1, HEAD_DIM), v_layers[layer])
            scores = jnp.einsum('bhd,bhsd->bhs', query.reshape(BATCH, HEADS, HEAD_DIM).astype(jnp.float32), k_layer.astype(jnp.float32))
            scores = jnp.where(valid, scores, -1e30)
            attn_probs = jax.nn.softmax(scores, axis=-1).astype(jnp.bfloat16)
            attn_out = jnp.einsum('bhs,bhsd->bhd', attn_probs.astype(jnp.float32), v_layer.astype(jnp.float32)).astype(jnp.bfloat16)
            residual = residual + matmul(attn_out.reshape(BATCH, D), w_o[layer]) + b_o[layer].astype(jnp.float32)
            hidden = layer_norm(residual, ln2_gain[layer], ln2_bias[layer])
            hidden_act = jax.nn.relu(matmul(hidden, w_fc1[layer]) + b_fc1[layer].astype(jnp.float32)).astype(jnp.bfloat16)
            residual = residual + matmul(hidden_act, w_fc2[layer]) + b_fc2[layer].astype(jnp.float32)
            new_k.append(k_layer)
            new_v.append(v_layer)
        final = layer_norm(residual, lnf_gain, lnf_bias)
        logits = jnp.dot(final, tok_table.T, preferred_element_type=jnp.float32)
        return (tuple(new_k), tuple(new_v)), logits

    init = (tuple(k_cache[layer] for layer in range(LAYERS)), tuple(v_cache[layer] for layer in range(LAYERS)))
    carry, logits = lax.scan(one_step, init, (tokens, jnp.arange(STEPS, dtype=jnp.int32)))
    return logits, jnp.stack(carry[0]), jnp.stack(carry[1])
```

```python
import functools
import math

import jax
import jax.numpy as jnp
from jax import lax
from jax.experimental import pallas as pl
from jax.experimental.pallas import tpu as pltpu
from jax.sharding import PartitionSpec as P

EPS = 1e-5
LANES = 128
SLOT = 8
MESH = pl.DeviceIdType.MESH
F32 = jnp.float32
BF16 = jnp.bfloat16
NT = (((1,), (1,)), ((), ()))


def dot(a, b):
    return jnp.dot(a, b, preferred_element_type=F32)


def dot_nt(a, b):
    return lax.dot_general(a, b, NT, preferred_element_type=F32)


def iota(shape, dim):
    return lax.broadcasted_iota(jnp.int32, shape, dim)


def layer_norm(x, gain, shift):
    mean = jnp.mean(x, axis=-1, keepdims=True)
    variance = jnp.mean(jnp.square(x - mean), axis=-1, keepdims=True)
    return ((x - mean) * lax.rsqrt(variance + EPS) * gain + shift).astype(BF16)


def decode_kernel(n, dims, pos_ref, tp_ref, tok_hbm, tok_tail, pos_tab, wa_ref, fs_ref, w2_ref, b1_ref, kc_hbm, vc_hbm,
                  lrecv, kv_out,
                  t_buf, e_buf, c_send, r_buf, w_buf, f_buf, k_buf, v_buf, h_src, h_buf, p_send, p_recv, l_send,
                  loc_sem, s_sem, r_sem, sw_sem, w1_sem, w2_sem, wd_sem):
    layers, seqs, heads, steps = dims
    me = lax.axis_index("dp")
    side = math.isqrt(n // 2)
    core = lax.rem(me, 2)
    cx = lax.rem(me // 2, side)
    cy = me // (2 * side)
    d = pos_tab.shape[1]
    head_dim = d // heads
    share = wa_ref.shape[1]
    wcols = wa_ref.shape[2]
    half = wcols // 2
    vocab_rows = tok_hbm.shape[0]
    main = e_buf.shape[0] - LANES
    ff = w2_ref.shape[0]
    ff_share = b1_ref.shape[1] // layers

    def dev(y, x, c):
        return (y * side + x) * 2 + c

    def remote(src, dst, ssem, rsem, peer):
        return pltpu.make_async_remote_copy(src_ref=src, dst_ref=dst, send_sem=ssem, recv_sem=rsem,
                                            device_id={"dp": peer}, device_id_type=MESH)

    def rows(ref, j, size):
        return ref.at[pl.ds(pl.multiple_of(j * size, SLOT), size)]

    e_copy = pltpu.make_async_copy(tok_hbm.at[pl.ds(0, main)], e_buf.at[pl.ds(0, main)], loc_sem.at[0])
    e_copy.start()
    cache_copies = []
    for l in range(layers):
        pair = (pltpu.make_async_copy(kc_hbm.at[l], k_buf.at[l], loc_sem.at[1 + 2 * l]),
                pltpu.make_async_copy(vc_hbm.at[l], v_buf.at[l], loc_sem.at[2 + 2 * l]))
        for copy in pair:
            copy.start()
        cache_copies.append(pair)

    barrier = pltpu.get_barrier_semaphore()

    def greet(r, carry):
        pl.semaphore_signal(barrier, inc=1, device_id={"dp": lax.rem(me + r, n)}, device_id_type=MESH)
        return carry

    lax.fori_loop(1, n, greet, 0)
    pl.semaphore_wait(barrier, n - 1)

    def broadcast(src, buf, size, k):
        def one(r, carry):
            remote(src, rows(buf, me, size), s_sem.at[k], r_sem.at[k], lax.rem(me + r, n)).start()
            return carry
        lax.fori_loop(1, n, one, 0)

    def scatter(src, buf, size, k):
        def one(r, carry):
            peer = lax.rem(me + r, n)
            remote(rows(src, peer, size), rows(buf, me, size), s_sem.at[k], r_sem.at[k], peer).start()
            return carry
        lax.fori_loop(1, n, one, 0)

    def most(buf, size):
        return buf.at[pl.ds(0, (n - 1) * size)]

    def arrived(buf, size, k):
        remote(most(buf, size), most(buf, size), s_sem.at[k], r_sem.at[k], me).wait_recv()

    def sent(buf, size, k):
        remote(most(buf, size), most(buf, size), s_sem.at[k], r_sem.at[k], me).wait_send()

    def own(buf, size):
        return pl.ds(pl.multiple_of(me * size, SLOT), size)

    def block_dev(color, along, across):
        if color == 0:
            return dev(lax.rem(cy + side - across, side), lax.rem(cx + side - along, side), core)
        return dev(lax.rem(cy + side - along, side), lax.rem(cx + side - across, side), core)

    def ring_peer(color, ring, step):
        if (color == 0) == (ring == 0):
            return dev(cy, lax.rem(cx + step, side), core)
        return dev(lax.rem(cy + step, side), cx, core)

    def wcol(color):
        return pl.ds(color * half, half)

    def wslot(l, color, j):
        return w_buf.at[l, pl.ds(pl.multiple_of(j * share, SLOT), share), wcol(color)]

    partner = dev(cy, cx, 1 - core)

    def gather_first(l):
        for color in range(2):
            for step in range(1, side):
                remote(wa_ref.at[l, :, wcol(color)], wslot(l, color, me), sw_sem.at[l, color],
                       w1_sem.at[l, color, step - 1], ring_peer(color, 0, step)).start()

    def gather_second(l):
        for along in range(side):
            for color in range(2):
                j = block_dev(color, along, 0)
                if along == 0:
                    src = wa_ref.at[l, :, wcol(color)]
                else:
                    src = wslot(l, color, j)
                    remote(src, src, sw_sem.at[l, color], w1_sem.at[l, color, along - 1], me).wait_recv()
                for step in range(1, side):
                    remote(src, wslot(l, color, j), sw_sem.at[l, color], w2_sem.at[l, color, along, step - 1],
                           ring_peer(color, 1, step)).start()
                remote(src, wslot(l, color, j), sw_sem.at[l, color], wd_sem.at[l], partner).start()

    def gather_third(l):
        w_buf[l, own(w_buf, share), :] = wa_ref[l]
        for across in range(1, side):
            for along in range(side):
                for color in range(2):
                    src = wslot(l, color, block_dev(color, along, across))
                    remote(src, src, sw_sem.at[l, color], w2_sem.at[l, color, along, across - 1], me).wait_recv()
                    remote(src, src, sw_sem.at[l, color], wd_sem.at[l], partner).start()

    def gather_wait(l):
        part = w_buf.at[l, pl.ds(0, n // 2 * share)]
        remote(part, part, sw_sem.at[l, 0], wd_sem.at[l], me).wait_recv()

    def gather_sent(l):
        for color in range(2):
            part = w_buf.at[l, pl.ds(0, (n - 1) * share), wcol(color)]
            remote(part, part, sw_sem.at[l, color], wd_sem.at[l], me).wait_send()

    TP, FC, EM, H0, P0 = 0, 1, 2, 3, 3 + layers + 1
    LG = P0 + layers

    broadcast(tp_ref, t_buf, SLOT, TP)
    t_buf[own(t_buf, SLOT), :] = tp_ref[...]
    gather_first(0)
    scatter(fs_ref, f_buf, share, FC)
    f_buf[own(f_buf, share), :] = fs_ref[own(fs_ref, share), :]
    e_buf[pl.ds(main, LANES), :] = tok_tail[...]
    e_copy.wait()
    arrived(t_buf, SLOT, TP)

    tokens = t_buf[:, 0:1] - me * vocab_rows
    places = t_buf[:, LANES // 2:LANES // 2 + 1] - me * pos_tab.shape[0]
    pick = (iota((n * SLOT, main + LANES), 1) == tokens).astype(F32).astype(BF16)
    c_send[:, 0:d] = dot(pick, e_buf[...]).astype(BF16)
    pick = (iota((n * SLOT, pos_tab.shape[0]), 1) == places).astype(F32).astype(BF16)
    c_send[:, d:2 * d] = dot(pick, pos_tab[...]).astype(BF16)
    scatter(c_send, r_buf, SLOT, EM)
    r_buf[own(r_buf, SLOT), :] = c_send[own(c_send, SLOT), :]

    gather_second(0)
    gather_first(1)

    arrived(f_buf, share, FC)
    vlane = layers * ff_share
    vcol = vlane // LANES * LANES
    count = 32
    select = (iota((count, LANES), 1) == iota((count, LANES), 0) + (vlane - vcol)).astype(F32).astype(BF16)
    vectors = dot_nt(select, f_buf[:, vcol:vcol + LANES])

    def vec(i, l):
        return vectors[layers * i + l:layers * i + l + 1, :]

    arrived(r_buf, SLOT, EM)
    found = jnp.sum(r_buf[...].astype(F32).reshape(n, SLOT, 2 * d), axis=0)
    x = found[:, 0:d] + found[:, d:2 * d]

    lane_head = iota((16, d), 1) // head_dim
    head_mask = lane_head == iota((16, d), 0)
    ff_lane = iota((n * SLOT, ff), 1)

    for l in range(layers):
        hidden = layer_norm(x, vec(0, l), vec(1, l))
        gather_third(l)
        gather_wait(l)
        q = ((dot(hidden, w_buf[l, :, 0:d]) + vec(2, l)) * head_dim ** -0.5).astype(BF16).astype(F32)
        k_new = (dot(hidden, w_buf[l, :, d:2 * d]) + vec(3, l)).astype(BF16)
        v_new = (dot(hidden, w_buf[l, :, 2 * d:3 * d]) + vec(4, l)).astype(BF16)
        kv_out[l, 0] = k_new
        kv_out[l, 1] = v_new
        v_wide = v_new.astype(F32)
        if l + 1 < layers:
            gather_second(l + 1)
        for copy in cache_copies[l]:
            copy.wait()
        outs = []
        for b in range(seqs):
            queries = jnp.concatenate(
                [jnp.where(head_mask, q[b * steps + t:b * steps + t + 1, :], 0.0) for t in range(steps)],
                axis=0).astype(BF16)
            scores = dot(queries, k_buf[l, b])
            scores = jnp.where(iota(scores.shape, 1) < pos_ref[b], scores, -1e30)
            fresh = dot_nt(queries, k_new)
            slot = iota(fresh.shape, 1) - b * steps
            fresh_ok = (slot >= 0) & (slot <= iota(fresh.shape, 0) // 16)
            fresh = jnp.where(fresh_ok, fresh, -1e30)
            top = jnp.maximum(jnp.max(scores, axis=-1, keepdims=True), jnp.max(fresh, axis=-1, keepdims=True))
            scores = jnp.exp(scores - top)
            fresh = jnp.exp(fresh - top)
            total = jnp.sum(scores, axis=-1, keepdims=True) + jnp.sum(fresh, axis=-1, keepdims=True)
            probs = (scores / total).astype(BF16)
            fresh = (fresh / total).astype(BF16).astype(F32)
            mixed = dot_nt(probs, v_buf[l, b])
            for t in range(steps):
                c = b * steps + t
                mixed = mixed + fresh[:, c:c + 1] * v_wide[c:c + 1, :]
            for t in range(steps):
                outs.append(jnp.sum(jnp.where(head_mask, mixed[16 * t:16 * t + 16, :], 0.0), axis=0, keepdims=True))
        outs.append(jnp.zeros((SLOT - seqs * steps, d), F32))
        attended = jnp.concatenate(outs, axis=0).astype(BF16)
        x = x + dot(attended, w_buf[l, :, 3 * d:4 * d]) + vec(5, l)

        hidden = layer_norm(x, vec(6, l), vec(7, l))
        h_src[l] = hidden
        broadcast(h_src.at[l], h_buf.at[l], SLOT, H0 + l)
        h_buf[l, own(h_buf, SLOT), :] = hidden
        arrived(h_buf.at[l], SLOT, H0 + l)
        act = jnp.maximum(dot(h_buf[l], f_buf[...]) + b1_pad(b1_ref, ff), 0.0)
        act = jnp.where((ff_lane >= l * ff_share) & (ff_lane < (l + 1) * ff_share), act, 0.0).astype(BF16)
        p_send[l] = dot(act, w2_ref[...])
        scatter(p_send.at[l], p_recv.at[l], SLOT, P0 + l)
        p_recv[l, own(p_recv, SLOT), :] = p_send[l, own(p_send, SLOT), :]
        arrived(p_recv.at[l], SLOT, P0 + l)
        x = x + jnp.sum(p_recv[l].reshape(n, SLOT, d), axis=0) + vec(8, l)

    final = layer_norm(x, vectors[9 * layers:9 * layers + 1, :], vectors[9 * layers + 1:9 * layers + 2, :])
    h_src[layers] = final
    broadcast(h_src.at[layers], h_buf.at[layers], SLOT, H0 + layers)
    h_buf[layers, own(h_buf, SLOT), :] = final
    arrived(h_buf.at[layers], SLOT, H0 + layers)

    def logits(c, carry):
        cols = pl.ds(pl.multiple_of(c * LANES, LANES), LANES)
        l_send[:, cols] = dot_nt(h_buf[layers], e_buf[cols, :])
        return carry

    lax.fori_loop(0, e_buf.shape[0] // LANES, logits, 0)
    scatter(l_send, lrecv, SLOT, LG)
    mine = pltpu.make_async_copy(rows(l_send, me, SLOT), rows(lrecv, me, SLOT), loc_sem.at[0])
    mine.start()

    sent(t_buf, SLOT, TP)
    sent(f_buf, share, FC)
    sent(r_buf, SLOT, EM)
    for l in range(layers):
        sent(h_buf.at[l], SLOT, H0 + l)
        sent(p_recv.at[l], SLOT, P0 + l)
        gather_sent(l)
    sent(h_buf.at[layers], SLOT, H0 + layers)
    mine.wait()
    arrived(lrecv, SLOT, LG)
    sent(lrecv, SLOT, LG)


def b1_pad(b1_ref, ff):
    return jnp.concatenate([b1_ref[...], jnp.zeros((1, ff - b1_ref.shape[1]), F32)], axis=1)


def finish_kernel(n, dims, vocab_rows, pos_ref, kv_ref, lrecv, kc_hbm, vc_hbm, logits, k_out, v_out, buf, in_sem, out_sem):
    layers, seqs, heads, steps = dims
    blocks = [(c, l, b) for l in range(layers) for b in range(seqs) for c in range(2)]
    loads = []
    for i, (c, l, b) in enumerate(blocks):
        src = (kc_hbm, vc_hbm)[c]
        loads.append(pltpu.make_async_copy(src.at[l, b], buf.at[i], in_sem.at[i]))
        loads[-1].start()
    stores = []
    per = n // len(blocks) + 1
    for i, (c, l, b) in enumerate(blocks):
        for j in range(i * per, min(n, (i + 1) * per)):
            part = lrecv[SLOT * j:SLOT * j + SLOT, 0:vocab_rows]
            for s in range(seqs):
                logits[s, :, vocab_rows * j:vocab_rows * (j + 1)] = part[s * steps:(s + 1) * steps, :]
        loads[i].wait()
        for t in range(steps):
            p = pos_ref[b] + t
            tile = pl.ds(pl.multiple_of(p // LANES * LANES, LANES), LANES)
            row = b * steps + t
            fresh = jnp.broadcast_to(kv_ref[l, c, :, row:row + 1], (buf.shape[1], LANES))
            hit = iota((buf.shape[1], LANES), 1) == lax.rem(p, LANES)
            old = buf[i, :, tile].astype(F32)
            buf[i, :, tile] = jnp.where(hit, fresh, old).astype(BF16)
        dst = (k_out, v_out)[c]
        stores.append(pltpu.make_async_copy(buf.at[i], dst.at[l, b], out_sem.at[i]))
        stores[-1].start()
    for copy in stores:
        copy.wait()


def solution(mesh):
    batch_axes = ("rep", "dp")
    mat_spec = P(None, "dp", None)
    vec_spec = P(None, "dp")
    in_specs = (P(None, batch_axes), P(batch_axes), P(None, batch_axes), P(None, batch_axes), P("dp", None), P("dp", None), vec_spec, vec_spec, mat_spec, mat_spec, mat_spec, vec_spec, vec_spec, vec_spec, mat_spec, vec_spec, vec_spec, vec_spec, mat_spec, vec_spec, mat_spec, vec_spec, P("dp"), P("dp"))
    out_specs = (P(None, batch_axes, None), P(None, batch_axes), P(None, batch_axes))
    n = mesh.shape["dp"]

    def body(tokens, start_pos, k_cache, v_cache, tok_table, pos_table, ln1_gain, ln1_bias, w_q, w_k, w_v, b_q, b_k, b_v, w_o, b_o, ln2_gain, ln2_bias, w_fc1, b_fc1, w_fc2, b_fc2, lnf_gain, lnf_bias):
        layers, seqs, heads, length, head_dim = k_cache.shape
        steps = tokens.shape[0]
        d = heads * head_dim
        share = w_q.shape[1]
        vocab_rows = tok_table.shape[0]
        main = vocab_rows // LANES * LANES
        count = seqs * steps
        ff_share = b_fc1.shape[1]
        ff = -(-(layers * ff_share + 32) // LANES) * LANES

        tok = jnp.pad(tokens.T.reshape(count, 1), ((0, SLOT - count), (0, 0)), constant_values=-1)
        place = (start_pos[:, None] + jnp.arange(steps, dtype=jnp.int32)[None, :]).reshape(count, 1)
        place = jnp.pad(place, ((0, SLOT - count), (0, 0)), constant_values=-1)
        tp = jnp.where(jnp.arange(LANES)[None, :] < LANES // 2, tok, place)
        wa = jnp.concatenate([w_q, w_k, w_v, w_o], axis=-1)
        vecs = jnp.concatenate([ln1_gain, ln1_bias, b_q, b_k, b_v, b_o, ln2_gain, ln2_bias, b_fc2,
                                lnf_gain[None], lnf_bias[None]], axis=0)
        fs = w_fc1.reshape(layers, share, n, ff_share).transpose(2, 1, 0, 3).reshape(n, share, layers * ff_share)
        vecs = jnp.broadcast_to(vecs.T[None], (n, share, vecs.shape[0]))
        fs = jnp.concatenate([fs, vecs], axis=-1)
        fs = jnp.pad(fs, ((0, 0), (0, 0), (0, ff - fs.shape[-1]))).reshape(n * share, ff)
        w2 = jnp.pad(w_fc2.reshape(layers * ff_share, d), ((0, ff - layers * ff_share), (0, 0)))
        b1 = b_fc1.astype(F32).reshape(1, layers * ff_share)
        tail = jnp.pad(tok_table[main:], ((0, main + LANES - vocab_rows), (0, 0)))
        kc = jnp.swapaxes(k_cache, 3, 4).reshape(layers, seqs, d, length)
        vc = jnp.swapaxes(v_cache, 3, 4).reshape(layers, seqs, d, length)

        dims = (layers, seqs, heads, steps)
        vmem = pl.BlockSpec(memory_space=pltpu.VMEM)
        anym = pl.BlockSpec(memory_space=pl.ANY)
        smem = pl.BlockSpec(memory_space=pltpu.SMEM)
        side = math.isqrt(n // 2)
        phases = 4 + 2 * layers + 1
        lrecv, kv_new = pl.pallas_call(
            functools.partial(decode_kernel, n, dims),
            out_shape=(jax.ShapeDtypeStruct((n * SLOT, main + LANES), F32),
                       jax.ShapeDtypeStruct((layers, 2, SLOT, d), BF16)),
            in_specs=[smem, vmem, anym, vmem, vmem, vmem, vmem, vmem, vmem, anym, anym],
            out_specs=(anym, vmem),
            scratch_shapes=[
                pltpu.VMEM((n * SLOT, LANES), jnp.int32),
                pltpu.VMEM((main + LANES, d), BF16),
                pltpu.VMEM((n * SLOT, 2 * d), BF16),
                pltpu.VMEM((n * SLOT, 2 * d), BF16),
                pltpu.VMEM((layers, n * share, 4 * d), BF16),
                pltpu.VMEM((n * share, ff), BF16),
                pltpu.VMEM((layers, seqs, d, length), BF16),
                pltpu.VMEM((layers, seqs, d, length), BF16),
                pltpu.VMEM((layers + 1, SLOT, d), BF16),
                pltpu.VMEM((layers + 1, n * SLOT, d), BF16),
                pltpu.VMEM((layers, n * SLOT, d), F32),
                pltpu.VMEM((layers, n * SLOT, d), F32),
                pltpu.VMEM((n * SLOT, main + LANES), F32),
                pltpu.SemaphoreType.DMA((1 + 2 * layers,)),
                pltpu.SemaphoreType.DMA((phases,)),
                pltpu.SemaphoreType.DMA((phases,)),
                pltpu.SemaphoreType.DMA((layers, 2)),
                pltpu.SemaphoreType.DMA((layers, 2, side - 1)),
                pltpu.SemaphoreType.DMA((layers, 2, side, side - 1)),
                pltpu.SemaphoreType.DMA((layers,)),
            ],
            compiler_params=pltpu.CompilerParams(collective_id=0, has_side_effects=True, vmem_limit_bytes=62 * 2 ** 20),
            name="decode",
        )(start_pos, tp, tok_table, tail, pos_table, wa, fs, w2, b1, kc, vc)

        kv_t = jnp.swapaxes(kv_new, 2, 3).astype(F32)
        logits, k_out, v_out = pl.pallas_call(
            functools.partial(finish_kernel, n, dims, vocab_rows),
            out_shape=(jax.ShapeDtypeStruct((seqs, steps, n * vocab_rows), F32),
                       jax.ShapeDtypeStruct(kc.shape, BF16), jax.ShapeDtypeStruct(vc.shape, BF16)),
            in_specs=[smem, vmem, vmem, anym, anym],
            out_specs=(vmem, anym, anym),
            scratch_shapes=[
                pltpu.VMEM((2 * layers * seqs, d, length), BF16),
                pltpu.SemaphoreType.DMA((2 * layers * seqs,)),
                pltpu.SemaphoreType.DMA((2 * layers * seqs,)),
            ],
            compiler_params=pltpu.CompilerParams(vmem_limit_bytes=60 * 2 ** 20),
            name="finish",
        )(start_pos, kv_t, lrecv, kc, vc)

        def unfold(cache):
            return jnp.swapaxes(cache.reshape(layers, seqs, heads, head_dim, length), 3, 4)

        return jnp.swapaxes(logits, 0, 1), unfold(k_out), unfold(v_out)

    return jax.shard_map(body, mesh=mesh, in_specs=in_specs, out_specs=out_specs, check_vma=False)
```
